32 devices in a mesh: clip: 4 (over y, x), head: 8 (over z, core).
Axes of the slice: x: 2, y: 2, z: 4, core: 2. Of those that a mesh axis runs over, the one named last changes fastest.
Arguments:
- queries: bfloat16 [8192, 4096], P(('clip', 'head')), may hold values from -6 to 6
- key_rows: bfloat16 [8192, 4096], P(('clip', 'head')), may hold values from -6 to 6
- value_rows: bfloat16 [8192, 4096], P(('clip', 'head')), may hold values from -6 to 6
- query_tangent: bfloat16 [8192, 4096], P(('clip', 'head')), may hold values from -6 to 6
- key_tangent: bfloat16 [8192, 4096], P(('clip', 'head')), may hold values from -6 to 6
- value_tangent: bfloat16 [8192, 4096], P(('clip', 'head')), may hold values from -6 to 6
- partners: int32 [8, 2], replicated, may hold values from 0 to 7, as said below
- cotangent: bfloat16 [8192, 3072], P('clip'), may hold values from -6 to 6
Outputs:
- attended: bfloat16 [8192, 4096], P(('clip', 'head'))
- attended_tangent: bfloat16 [8192, 4096], P(('clip', 'head'))
- weight_grad: float32 [3072, 4096], P('clip', 'head')
The draws below stay inside these ranges and needn't reach their ends.
Inputs may be any that keep to these rules, and one draw needn't show every extreme that they name: `partners`: for clip c the two entries are distinct clips (c - d) mod 8 with 1 <= d <= 2 + c % 2.
All inputs are finite; a program needn't handle non-finite values.
Results may differ from the reference program's by a relative error of at most 0.0051.
Values may be sent and summed in bfloat16 or wider, within the bound.
A program may use at most 192 MiB of HBM per device.

```python
import jax
import jax.numpy as jnp
from jax import lax

HEADS = 32
HDIM = 128
DOUT = 3072
CLIP = 1024
CLIPS_DEV = 2
CLIPS = 8
TOKENS = 8192
QW = 4096


def shared_rows(key):
    base_q = jnp.clip(jax.random.normal(jax.random.fold_in(key, 11), (TOKENS, QW), jnp.float32), -6.0, 6.0)
    base_k = jnp.clip(jax.random.normal(jax.random.fold_in(key, 12), (TOKENS, QW), jnp.float32), -6.0, 6.0)
    return (base_q, base_k)


def draw_queries(key, part):
    return shared_rows(key)[0].astype(jnp.bfloat16)


def draw_key_rows(key, part):
    return shared_rows(key)[1].astype(jnp.bfloat16)


def draw_partners(key, part):
    clip_ids = jnp.arange(CLIPS, dtype=jnp.int32)
    gap_reach = CLIPS_DEV + clip_ids % CLIPS_DEV
    first_gap = jax.random.randint(jax.random.fold_in(key, 21), (CLIPS,), 0, 1 << 20) % gap_reach + 1
    gap_step = jax.random.randint(jax.random.fold_in(key, 22), (CLIPS,), 0, 1 << 20) % (gap_reach - 1) + 1
    second_gap = (first_gap - 1 + gap_step) % gap_reach + 1
    return jnp.stack([(clip_ids - first_gap) % CLIPS, (clip_ids - second_gap) % CLIPS], axis=1).astype(jnp.int32)


def spiked(result, key, source, target, shards_of, factor):
    def block_of(axis_at):
        return (jnp.arange(result.shape[axis_at]) // (result.shape[axis_at] // shards_of)).reshape((-1,) + (1,) * (result.ndim - 1 - axis_at))

    near = jax.random.permutation(key, shards_of)[block_of(target)]
    other_side = (block_of(target) + shards_of // 2) % shards_of
    return jnp.where((block_of(source) == near) | (block_of(source) == other_side), factor * result, result)


def steps_of(key, shape, shards, smallest, top_value):
    loudness = 1.0
    for dim, parts in shards:
        draws = jax.random.uniform(jax.random.fold_in(jax.random.fold_in(key, 6), dim), (parts,), jnp.float32, smallest / len(shards), top_value / len(shards))
        loudness = loudness * jnp.repeat(jnp.exp(draws), shape[dim] // parts).reshape((-1,) + (1,) * (len(shape) - 1 - dim))
    return loudness


def gaussian(stream_key, dims, width, limit, split=(), kind=jnp.bfloat16):
    entries = width * jax.random.normal(stream_key, dims, jnp.float32)
    if split:
        entries = entries * steps_of(stream_key, dims, split, -0.22, 0.18)
    return jnp.clip(entries, -limit, limit).astype(kind)


def bell_draw_with(own_key, extent, width, reach, cuts, heavy, kind=jnp.bfloat16):
    result = width * jax.random.normal(own_key, extent, jnp.float32)
    if cuts:
        result = result * steps_of(own_key, extent, cuts, -0.22, 0.18)
    return jnp.clip(spiked(result, jax.random.fold_in(own_key, 3), *heavy), -reach, reach).astype(kind)


def setup_inputs(seed: int = 0) -> dict:
    arg_keys = jax.random.split(jax.random.key(seed), 9)
    queries = draw_queries(jax.random.fold_in(arg_keys[8], 71), 0)
    key_rows = draw_key_rows(jax.random.fold_in(arg_keys[8], 71), 0)
    value_rows = gaussian(arg_keys[2], (TOKENS, QW), 1.0, 6.0, ((0, 32),))
    query_tangent = gaussian(arg_keys[3], (TOKENS, QW), 1.0, 6.0, ((0, 32),))
    key_tangent = gaussian(arg_keys[4], (TOKENS, QW), 1.0, 6.0, ((0, 32),))
    value_tangent = gaussian(arg_keys[5], (TOKENS, QW), 1.0, 6.0, ((0, 32),))
    partners = draw_partners(jax.random.fold_in(arg_keys[8], 71), 0)
    cotangent = bell_draw_with(arg_keys[7], (TOKENS, DOUT), 1.0, 6.0, ((0, 4),), (0, 1, 4, 2.0))
    return dict(queries=queries, key_rows=key_rows, value_rows=value_rows, query_tangent=query_tangent, key_tangent=key_tangent, value_tangent=value_tangent, partners=partners, cotangent=cotangent)


def attend_head(query_part, qtan_part, key_win, value_win, ktan_win, vtan_win):
    score_scale = HDIM ** -0.5
    scores = jnp.dot(query_part, key_win.T, preferred_element_type=jnp.float32) * score_scale
    score_tan = (jnp.dot(qtan_part, key_win.T, preferred_element_type=jnp.float32)
                 + jnp.dot(query_part, ktan_win.T, preferred_element_type=jnp.float32)) * score_scale
    row_max = jnp.max(scores, axis=-1, keepdims=True)
    raw_weights = jnp.exp(scores - row_max)
    row_total = jnp.sum(raw_weights, axis=-1, keepdims=True)
    probability = raw_weights / row_total
    tangent_mean = jnp.sum(probability * score_tan, axis=-1, keepdims=True)
    prob_tangent = probability * (score_tan - tangent_mean)
    prob_low = probability.astype(jnp.bfloat16)
    tangent_low = prob_tangent.astype(jnp.bfloat16)
    result_out = jnp.dot(prob_low, value_win, preferred_element_type=jnp.float32)
    tangent_out = (jnp.dot(tangent_low, value_win, preferred_element_type=jnp.float32)
                   + jnp.dot(prob_low, vtan_win, preferred_element_type=jnp.float32))
    return result_out.astype(jnp.bfloat16), tangent_out.astype(jnp.bfloat16)


def reference(queries, key_rows, value_rows, query_tangent, key_tangent, value_tangent, partners, cotangent):
    def split_heads(array):
        return array.reshape(CLIPS, CLIP, HEADS, HDIM)

    queries4 = split_heads(queries)
    keys4 = split_heads(key_rows)
    values4 = split_heads(value_rows)
    qtan4 = split_heads(query_tangent)
    ktan4 = split_heads(key_tangent)
    vtan4 = split_heads(value_tangent)

    def one_clip(clip_index):
        partner_row = partners[clip_index]
        chosen = jnp.stack([clip_index, partner_row[0], partner_row[1]]).astype(jnp.int32)

        def window(array):
            return jnp.take(array, chosen, axis=0).reshape(3 * CLIP, HEADS, HDIM)

        key_win = window(keys4)
        value_win = window(values4)
        ktan_win = window(ktan4)
        vtan_win = window(vtan4)
        query_clip = queries4[clip_index]
        qtan_clip = qtan4[clip_index]

        def one_head(head_index):
            return attend_head(jnp.take(query_clip, head_index, axis=1), jnp.take(qtan_clip, head_index, axis=1),
                               jnp.take(key_win, head_index, axis=1), jnp.take(value_win, head_index, axis=1),
                               jnp.take(ktan_win, head_index, axis=1), jnp.take(vtan_win, head_index, axis=1))

        head_out, head_tan = lax.map(one_head, jnp.arange(HEADS, dtype=jnp.int32))
        return jnp.transpose(head_out, (1, 0, 2)), jnp.transpose(head_tan, (1, 0, 2))

    clip_out, clip_tan = lax.map(one_clip, jnp.arange(CLIPS, dtype=jnp.int32))
    attended = clip_out.reshape(TOKENS, QW)
    attended_tangent = clip_tan.reshape(TOKENS, QW)
    weight_grad = lax.dot_general(cotangent, attended, (((0,), (0,)), ((), ())), preferred_element_type=jnp.float32)
    return attended, attended_tangent, weight_grad
```

```python
import functools
import math

import jax
import jax.numpy as jnp
from jax import lax
from jax.experimental import pallas as pl
from jax.experimental.pallas import tpu as pltpu
from jax.sharding import PartitionSpec as P

HDIM = 128
CLIP = 1024
AHEAD = 4
NT = (((1,), (1,)), ((), ()))
MESH = pl.DeviceIdType.MESH


def attend_rows(both, wk, wv, scale):
    f32 = jnp.float32
    scores = lax.dot_general(both[:, HDIM:], wk[:, :HDIM], NT, preferred_element_type=f32)
    score_tan = lax.dot_general(both, wk[...], NT, preferred_element_type=f32)
    row_max = jnp.max(scores, axis=1, keepdims=True)
    weights = jnp.exp2((scores - row_max) * (scale * math.log2(math.e)))
    inverse = 1.0 / jnp.sum(weights, axis=1, keepdims=True)
    mean = jnp.sum(weights * score_tan, axis=1, keepdims=True) * inverse
    low = weights.astype(jnp.bfloat16)
    tan_low = (weights * (score_tan - mean)).astype(jnp.bfloat16)
    first = jnp.dot(low, wv[...], preferred_element_type=f32)
    second = jnp.dot(tan_low, wv[:, :HDIM], preferred_element_type=f32)
    out = first[:, :HDIM] * inverse
    tan = (first[:, HDIM:] + second * scale) * inverse
    return out.astype(jnp.bfloat16), tan.astype(jnp.bfloat16)


KEYS, VALUES, QUERIES = (0, 1), (2, 3), (4, 5)


def exchange_kernel(n, clips, heads, partners, *refs):
    args, cotangent, (out, tan, grad) = refs[:6], refs[6], refs[7:10]
    refs = refs[10:]
    kk, vv, qq, oo = (refs[i * heads : (i + 1) * heads] for i in range(4))
    wk, wv, cot, flipped, terms, others = refs[4 * heads : 4 * heads + 6]
    send, recv, local, fsend, frecv, osend, orecv, olocal, gsend, grecv, csem = refs[4 * heads + 6 :]
    piece = args[0].shape[0]
    rows = n * piece
    wide = cot.shape[1] // clips
    me, group = lax.axis_index("head"), lax.axis_index("clip")
    after, before = lax.rem(group + 1, clips), lax.rem(group + clips - 1, clips)
    if n & (n - 1) == 0:
        steps = [d for bit in range(n.bit_length() - 2, -1, -1) for d in range(1 << bit, 2 << bit)]
        peers = [(me ^ d, me ^ d) for d in steps]
    else:
        peers = [(lax.rem(me + d, n), lax.rem(me + n - d, n)) for d in range(1, n)]
    groups = [(lax.rem(group + d, clips), lax.rem(group + clips - d, clips)) for d in range(1, clips)]

    barrier = pltpu.get_barrier_semaphore()
    for to, _ in peers:
        pl.semaphore_signal(barrier, inc=1, device_id={"head": to}, device_id_type=MESH)
    for to, _ in groups:
        pl.semaphore_signal(barrier, inc=1, device_id={"clip": to}, device_id_type=MESH)
    pl.semaphore_wait(barrier, n - 1 + clips - 1)

    def landing(head, t, source):
        buffer, base = ((kk, rows), (vv, rows), (qq, 0))[t // 2]
        at = pl.ds(pl.multiple_of(base + source * piece, piece), piece)
        return buffer[head].at[at, pl.ds(HDIM * (t % 2), HDIM)]

    def column(head, t, owner):
        at = pl.ds(pl.multiple_of((owner * heads + head) * HDIM, HDIM), HDIM)
        return args[t].at[:, at]

    def outgoing(head, t, to):
        return pltpu.make_async_remote_copy(
            src_ref=column(head, t, to),
            dst_ref=landing(head, t, me),
            send_sem=send.at[head, t, to],
            recv_sem=recv.at[head, t, me],
            device_id={"head": to},
            device_id_type=MESH,
        )

    def incoming(head, t, source):
        return pltpu.make_async_remote_copy(
            src_ref=column(head, t, source),
            dst_ref=landing(head, t, source),
            send_sem=send.at[head, t, source],
            recv_sem=recv.at[head, t, source],
            device_id={"head": source},
            device_id_type=MESH,
        )

    def stay(head, t):
        return pltpu.make_async_copy(column(head, t, me), landing(head, t, me), local.at[head, t])

    def forward(head, which):
        buffer = (kk, vv)[which][head]
        return pltpu.make_async_remote_copy(
            src_ref=buffer.at[pl.ds(rows, rows)],
            dst_ref=buffer.at[pl.ds(0, rows)],
            send_sem=fsend.at[head, which],
            recv_sem=frecv.at[head, which],
            device_id={"clip": after},
            device_id_type=MESH,
        )

    def issue(stage):
        head, tensors = stage
        for t in tensors:
            for to, _ in peers:
                outgoing(head, t, to).start()
            stay(head, t).start()

    def arrive(stage):
        head, tensors = stage
        for t in tensors:
            stay(head, t).wait()
            for _, source in peers:
                incoming(head, t, source).wait_recv()

    def result_rows(head, which, owner):
        at = pl.ds(pl.multiple_of(owner * piece, piece), piece)
        return oo[head].at[at, pl.ds(HDIM * which, HDIM)]

    def result_home(head, which, maker):
        at = pl.ds(pl.multiple_of((maker * heads + head) * HDIM, HDIM), HDIM)
        return (out, tan)[which].at[:, at]

    def give(head, which, to):
        return pltpu.make_async_remote_copy(
            src_ref=result_rows(head, which, to),
            dst_ref=result_home(head, which, me),
            send_sem=osend.at[head, which, to],
            recv_sem=orecv.at[head, which, me],
            device_id={"head": to},
            device_id_type=MESH,
        )

    def take(head, which, maker):
        return pltpu.make_async_remote_copy(
            src_ref=result_rows(head, which, maker),
            dst_ref=result_home(head, which, maker),
            send_sem=osend.at[head, which, maker],
            recv_sem=orecv.at[head, which, maker],
            device_id={"head": maker},
            device_id_type=MESH,
        )

    def keep(head, which):
        return pltpu.make_async_copy(
            result_rows(head, which, me), result_home(head, which, me), olocal.at[head, which]
        )

    def hand_out(head, owner):
        @pl.when(owner == me)
        def _():
            for which in range(2):
                keep(head, which).start()

        @pl.when(owner != me)
        def _():
            for which in range(2):
                give(head, which, owner).start()

    clip_count = rows // CLIP
    block_rows = min(256, piece)
    per_clip, per_piece = CLIP // block_rows, piece // block_rows
    total_clips = clip_count * clips
    home = me * piece // CLIP

    def block_of(step):
        within = lax.rem(home + 1 + step // per_clip, clip_count)
        return within * per_clip + lax.rem(step, per_clip)

    def is_one(value):
        return jnp.full((16, 2 * HDIM), jnp.where(value, 1.0, 0.0), jnp.float32).astype(jnp.bfloat16)

    def attend(head):
        def one_clip(turn, _):
            within = lax.rem(home + 1 + turn, clip_count)
            own = clip_count + within
            clip_id = group * clip_count + within
            gaps = [lax.rem(clip_id - partners[clip_id, i] + total_clips, total_clips) for i in range(2)]
            near, far = jnp.minimum(*gaps) == 1, jnp.maximum(*gaps) == 2
            flags = [is_one(near), is_one(jnp.logical_not(near)), is_one(far), is_one(jnp.logical_not(far))]
            for place in range(3):
                at = pl.ds(place * CLIP, CLIP)
                for window, held in ((wk, kk[head]), (wv, vv[head])):

                    def clip_back(gap):
                        row = pl.multiple_of(lax.max(own - gap, 0) * CLIP, CLIP)
                        return held[pl.ds(row, CLIP), :].reshape(CLIP // 16, 16, 2 * HDIM)

                    if place == 0:
                        window[at, :] = held[pl.ds(pl.multiple_of(own * CLIP, CLIP), CLIP), :]
                    else:
                        flag = (place - 1) * 2
                        mixed = clip_back(place) * flags[flag] + clip_back(place + 1) * flags[flag + 1]
                        window[at, :] = mixed.reshape(CLIP, 2 * HDIM)

            def one_block(block, _):
                row = within * CLIP + block * block_rows
                at = pl.ds(pl.multiple_of(row, block_rows), block_rows)
                step = turn * per_clip + block
                result = attend_rows(qq[head][at, :], wk, wv, HDIM**-0.5)
                oo[head][at, :HDIM], oo[head][at, HDIM:] = result

                @pl.when(jnp.logical_and(step > 0, lax.rem(step, per_piece) == 0))
                def _():
                    hand_out(head, block_of(step - 1) // per_piece)

                return 0

            return lax.fori_loop(0, per_clip, one_block, 0)

        lax.fori_loop(0, clip_count, one_clip, 0)

    tile = 256 if cot.shape[1] % 256 == 0 else HDIM

    def multiply(head):
        flipped[...] = oo[head][:, :HDIM].T

        def one_tile(j, _):
            at = pl.ds(pl.multiple_of(j * tile, tile), tile)
            terms[head % 2, :, at] = jnp.dot(
                flipped[...], cot[:, at], preferred_element_type=jnp.float32
            )
            return 0

        lax.fori_loop(0, cot.shape[1] // tile, one_tile, 0)

    def share(owner):
        return pl.ds(pl.multiple_of(owner * wide, HDIM), wide)

    def give_term(head, to, source):
        return pltpu.make_async_remote_copy(
            src_ref=terms.at[head % 2, :, share(to)],
            dst_ref=others.at[head, source],
            send_sem=gsend.at[head, to],
            recv_sem=grecv.at[head, source],
            device_id={"clip": to},
            device_id_type=MESH,
        )

    def reduce_terms(head):
        total = terms[head % 2, :, share(group)]
        for _, source in groups:
            give_term(head, source, source).wait_recv()
            total = total + others[head, source]
        grad[:, head * HDIM : (head + 1) * HDIM] = total.T

    stages = []
    for head in range(heads):
        stages += [(head, KEYS), (head, VALUES)]
        if head:
            stages.append((head - 1, QUERIES))
    stages.append((heads - 1, QUERIES))
    load = pltpu.make_async_copy(cotangent, cot, csem)
    for stage in stages[:AHEAD]:
        issue(stage)
    load.start()
    for number, stage in enumerate(stages):
        arrive(stage)
        if number + AHEAD < len(stages):
            issue(stages[number + AHEAD])
        head, tensors = stage
        if tensors is not QUERIES:
            forward(head, tensors[0] // 2).start()
            continue
        for which in range(2):
            forward(head, which).wait_recv()
        attend(head)
        if head == 0:
            load.wait()
        if head >= 2:
            for to, _ in groups:
                give_term(head - 2, to, group).wait_send()
        multiply(head)
        hand_out(head, block_of(rows // block_rows - 1) // per_piece)
        for to, _ in groups:
            give_term(head, to, group).start()
        if head:
            reduce_terms(head - 1)
    reduce_terms(heads - 1)
    for head in range(heads):
        for which in range(2):
            forward(head, which).wait_send()
            keep(head, which).wait()
            for to, maker in peers:
                give(head, which, to).wait_send()
                take(head, which, maker).wait_recv()
        for t in range(6):
            for to, _ in peers:
                outgoing(head, t, to).wait_send()
    for head in range(max(heads - 2, 0), heads):
        for to, _ in groups:
            give_term(head, to, group).wait_send()


def on_device(
    queries, key_rows, value_rows, query_tangent, key_tangent, value_tangent, partners, cotangent
):
    n, clips = lax.axis_size("head"), lax.axis_size("clip")
    rows, cols = queries.shape[0] * n, queries.shape[1] // n
    heads = cols // HDIM
    width = cotangent.shape[1]
    args = (key_rows, key_tangent, value_rows, value_tangent, query_tangent, queries)
    low, f32 = jnp.bfloat16, jnp.float32
    like = jax.ShapeDtypeStruct(queries.shape, low)
    dma = pltpu.SemaphoreType.DMA
    hbm = pl.BlockSpec(memory_space=pl.ANY)
    return pl.pallas_call(
        functools.partial(exchange_kernel, n, clips, heads),
        out_shape=(like, like, jax.ShapeDtypeStruct((width // clips, cols), f32)),
        in_specs=[pl.BlockSpec(memory_space=pltpu.SMEM)] + [hbm] * 7,
        out_specs=[hbm, hbm, pl.BlockSpec(memory_space=pltpu.VMEM)],
        scratch_shapes=[pltpu.VMEM((2 * rows, 2 * HDIM), low)] * (2 * heads)
        + [pltpu.VMEM((rows, 2 * HDIM), low)] * (2 * heads)
        + [pltpu.VMEM((3 * CLIP, 2 * HDIM), low)] * 2
        + [
            pltpu.VMEM((rows, width), low),
            pltpu.VMEM((HDIM, rows), low),
            pltpu.VMEM((2, HDIM, width), f32),
            pltpu.VMEM((heads, clips, HDIM, width // clips), f32),
        ]
        + [dma((heads, 6, n)), dma((heads, 6, n)), dma((heads, 6)), dma((heads, 2)), dma((heads, 2))]
        + [dma((heads, 2, n)), dma((heads, 2, n)), dma((heads, 2))]
        + [dma((heads, clips)), dma((heads, clips)), dma],
        compiler_params=pltpu.CompilerParams(
            collective_id=0, has_side_effects=True, vmem_limit_bytes=63 * 1024 * 1024
        ),
        cost_estimate=pl.CostEstimate(
            flops=12 * rows * cols * 3 * CLIP + 2 * rows * cols * width,
            bytes_accessed=16 * rows * cols * 2 + rows * width * 2,
            transcendentals=rows * heads * 3 * CLIP,
        ),
    )(partners, *args, cotangent)


def solution(mesh):
    tokens = P(("clip", "head"), None)
    return jax.shard_map(
        on_device,
        mesh=mesh,
        in_specs=(tokens,) * 6 + (P(), P("clip", None)),
        out_specs=(tokens, tokens, P("clip", "head")),
        check_vma=False,
    )
```

```python
import functools
import math

import jax
import jax.numpy as jnp
from jax import lax
from jax.experimental import pallas as pl
from jax.experimental.pallas import tpu as pltpu
from jax.sharding import PartitionSpec as P

HDIM = 128
CLIP = 1024
AHEAD = 4
NT = (((1,), (1,)), ((), ()))
MESH = pl.DeviceIdType.MESH


def attend_rows(both, wk, wv, scale):
    f32 = jnp.float32
    scores = lax.dot_general(both[:, HDIM:], wk[:, :HDIM], NT, preferred_element_type=f32)
    score_tan = lax.dot_general(both, wk[...], NT, preferred_element_type=f32)
    row_max = jnp.max(scores, axis=1, keepdims=True)
    weights = jnp.exp2((scores - row_max) * (scale * math.log2(math.e)))
    inverse = 1.0 / jnp.sum(weights, axis=1, keepdims=True)
    mean = jnp.sum(weights * score_tan, axis=1, keepdims=True) * inverse
    low = weights.astype(jnp.bfloat16)
    tan_low = (weights * (score_tan - mean)).astype(jnp.bfloat16)
    first = jnp.dot(low, wv[...], preferred_element_type=f32)
    second = jnp.dot(tan_low, wv[:, :HDIM], preferred_element_type=f32)
    out = first[:, :HDIM] * inverse
    tan = (first[:, HDIM:] + second * scale) * inverse
    return out.astype(jnp.bfloat16), tan.astype(jnp.bfloat16)


def exchange_kernel(n, clips, heads, partners, *refs):
    args, cotangent, (out, tan, grad) = refs[:6], refs[6], refs[7:10]
    kk, vv, qq, oo, wk, wv, cot, flipped, terms, others, chosen = refs[10:21]
    send, recv, local, fsend, frecv, osend, orecv, olocal, gsend, grecv, csem = refs[21:]
    piece = args[0].shape[0]
    rows = n * piece
    wide = cot.shape[1] // clips
    me, group = lax.axis_index("head"), lax.axis_index("clip")
    after = lax.rem(group + 1, clips)
    if n & (n - 1) == 0:
        steps = [d for bit in range(n.bit_length() - 2, -1, -1) for d in range(1 << bit, 2 << bit)]
        peers = [(me ^ d, me ^ d) for d in steps]
    else:
        peers = [(lax.rem(me + d, n), lax.rem(me + n - d, n)) for d in range(1, n)]
    groups = [(lax.rem(group + d, clips), lax.rem(group + clips - d, clips)) for d in range(1, clips)]

    barrier = pltpu.get_barrier_semaphore()
    for to, _ in peers:
        pl.semaphore_signal(barrier, inc=1, device_id={"head": to}, device_id_type=MESH)
    for to, _ in groups:
        pl.semaphore_signal(barrier, inc=1, device_id={"clip": to}, device_id_type=MESH)
    pl.semaphore_wait(barrier, n - 1 + clips - 1)

    def whole(owner, head, count):
        return pl.ds(pl.multiple_of((owner * heads + head) * HDIM, HDIM), count * HDIM)

    def held(part, head, count):
        return pl.ds((heads * part + head) * HDIM, count * HDIM)

    def piece_of(base, source):
        return pl.ds(pl.multiple_of(base + source * piece, piece), piece)

    def landing(batch, source):
        t, head, count = batch
        buffer, base = ((kk, rows), (vv, rows), (qq, 0))[t // 2]
        return buffer.at[piece_of(base, source), held(t % 2, head, count)]

    def column(batch, owner):
        t, head, count = batch
        return args[t].at[:, whole(owner, head, count)]

    def outgoing(batch, to):
        t, head, count = batch
        return pltpu.make_async_remote_copy(
            src_ref=column(batch, to),
            dst_ref=landing(batch, me),
            send_sem=send.at[head, t, to],
            recv_sem=recv.at[head, t, me],
            device_id={"head": to},
            device_id_type=MESH,
        )

    def incoming(batch, source):
        t, head, count = batch
        return pltpu.make_async_remote_copy(
            src_ref=column(batch, source),
            dst_ref=landing(batch, source),
            send_sem=send.at[head, t, source],
            recv_sem=recv.at[head, t, source],
            device_id={"head": source},
            device_id_type=MESH,
        )

    def stay(batch):
        t, head, count = batch
        return pltpu.make_async_copy(column(batch, me), landing(batch, me), local.at[head, t])

    def forward(batch):
        t, head, count = batch
        buffer, cols = (kk, vv)[t // 2], held(t % 2, head, count)
        return pltpu.make_async_remote_copy(
            src_ref=buffer.at[pl.ds(rows, rows), cols],
            dst_ref=buffer.at[pl.ds(0, rows), cols],
            send_sem=fsend.at[head, t],
            recv_sem=frecv.at[head, t],
            device_id={"clip": after},
            device_id_type=MESH,
        )

    def issue(stage):
        for batch in stage:
            for to, _ in peers:
                outgoing(batch, to).start()
            stay(batch).start()

    def arrive(stage):
        for batch in stage:
            stay(batch).wait()
            for _, source in peers:
                incoming(batch, source).wait_recv()
            if batch[0] < 4:
                forward(batch).start()

    def result_rows(lot, which, owner):
        head, count = lot
        at = pl.ds(pl.multiple_of(owner * piece, piece), piece)
        return oo.at[at, held(which, head, count)]

    def result_home(lot, which, maker):
        return (out, tan)[which].at[:, whole(maker, *lot)]

    def give(lot, which, to):
        return pltpu.make_async_remote_copy(
            src_ref=result_rows(lot, which, to),
            dst_ref=result_home(lot, which, me),
            send_sem=osend.at[lot[0], which, to],
            recv_sem=orecv.at[lot[0], which, me],
            device_id={"head": to},
            device_id_type=MESH,
        )

    def take(lot, which, maker):
        return pltpu.make_async_remote_copy(
            src_ref=result_rows(lot, which, maker),
            dst_ref=result_home(lot, which, maker),
            send_sem=osend.at[lot[0], which, maker],
            recv_sem=orecv.at[lot[0], which, maker],
            device_id={"head": maker},
            device_id_type=MESH,
        )

    def keep(lot, which):
        return pltpu.make_async_copy(
            result_rows(lot, which, me), result_home(lot, which, me), olocal.at[lot[0], which]
        )

    def hand_out(lot, owner):
        @pl.when(owner == me)
        def _():
            for which in range(2):
                keep(lot, which).start()

        @pl.when(owner != me)
        def _():
            for which in range(2):
                give(lot, which, owner).start()

    clip_count = rows // CLIP
    block_rows = min(256, piece)
    per_clip, per_piece = CLIP // block_rows, piece // block_rows
    total_clips = clip_count * clips
    home = me * piece // CLIP

    def block_of(step):
        within = lax.rem(home + 1 + step // per_clip, clip_count)
        return within * per_clip + lax.rem(step, per_clip)

    def is_one(value):
        return jnp.full((16, HDIM), jnp.where(value, 1.0, 0.0), jnp.float32).astype(jnp.bfloat16)

    def attend(head, lot):
        def one_clip(turn, _):
            within = lax.rem(home + 1 + turn, clip_count)
            own = clip_count + within
            clip_id = group * clip_count + within
            gaps = [lax.rem(clip_id - chosen[i, clip_id] + total_clips, total_clips) for i in range(2)]
            near, far = jnp.minimum(*gaps) == 1, jnp.maximum(*gaps) == 2
            flags = [is_one(near), is_one(jnp.logical_not(near)), is_one(far), is_one(jnp.logical_not(far))]
            for place in range(3):
                at = pl.ds(place * CLIP, CLIP)
                for window, rows_held in ((wk, kk), (wv, vv)):
                    for part in range(2):

                        def clip_back(gap):
                            row = pl.multiple_of(lax.max(own - gap, 0) * CLIP, CLIP)
                            return rows_held[pl.ds(row, CLIP), held(part, head, 1)]

                        if place == 0:
                            mixed = clip_back(0)
                        else:
                            first, second = (
                                clip_back(place + i).reshape(CLIP // 16, 16, HDIM) * flags[place * 2 - 2 + i]
                                for i in range(2)
                            )
                            mixed = (first + second).reshape(CLIP, HDIM)
                        window[at, part * HDIM : (part + 1) * HDIM] = mixed

            def one_block(block, _):
                row = within * CLIP + block * block_rows
                at = pl.ds(pl.multiple_of(row, block_rows), block_rows)
                step = turn * per_clip + block
                both = jnp.concatenate([qq[at, held(part, head, 1)] for part in range(2)], axis=1)
                result = attend_rows(both, wk, wv, HDIM**-0.5)
                oo[at, held(0, head, 1)], oo[at, held(1, head, 1)] = result

                if lot is not None:

                    @pl.when(jnp.logical_and(step > 0, lax.rem(step, per_piece) == 0))
                    def _():
                        hand_out(lot, block_of(step - 1) // per_piece)

                return 0

            return lax.fori_loop(0, per_clip, one_block, 0)

        lax.fori_loop(0, clip_count, one_clip, 0)

    tile = 256 if cot.shape[1] % 256 == 0 else HDIM

    def multiply(head):
        flipped[...] = oo[:, held(0, head, 1)].T

        def one_tile(j, _):
            at = pl.ds(pl.multiple_of(j * tile, tile), tile)
            terms[head % 2, :, at] = jnp.dot(
                flipped[...], cot[:, at], preferred_element_type=jnp.float32
            )
            return 0

        lax.fori_loop(0, cot.shape[1] // tile, one_tile, 0)

    def share(owner):
        return pl.ds(pl.multiple_of(owner * wide, HDIM), wide)

    def give_term(head, to, source):
        return pltpu.make_async_remote_copy(
            src_ref=terms.at[head % 2, :, share(to)],
            dst_ref=others.at[head, source],
            send_sem=gsend.at[head, to],
            recv_sem=grecv.at[head, source],
            device_id={"clip": to},
            device_id_type=MESH,
        )

    def reduce_terms(head):
        total = terms[head % 2, :, share(group)]
        for _, source in groups:
            give_term(head, source, source).wait_recv()
            total = total + others[head, source]
        grad[:, head * HDIM : (head + 1) * HDIM] = total.T

    stages, ready = [], []
    for head in range(heads + 1):
        if head < heads:
            stages += [[(t, head, 1), (t + 1, head, 1)] for t in (0, 2)]
            ready += [None, None]
        if head:
            stages.append([(4, head - 1, 1), (5, head - 1, 1)])
            ready.append(head - 1)

    lots = [(i, 1) for i in range(heads)]
    if heads % 2 == 0:
        for i in range(0, heads - 2, 2):
            lots[i], lots[i + 1] = None, (i, 2)

    def compute(head):
        if head == 0:
            choose.wait()
            load.wait()
        for t in range(4):
            forward((t, head, 1)).wait_recv()
        attend(head, lots[head])
        if head >= 2:
            for to, _ in groups:
                give_term(head - 2, to, group).wait_send()
        multiply(head)
        if lots[head] is not None:
            hand_out(lots[head], block_of(rows // block_rows - 1) // per_piece)
        for to, _ in groups:
            give_term(head, to, group).start()
        if head:
            reduce_terms(head - 1)

    load = pltpu.make_async_copy(cotangent, cot, csem.at[0])
    choose = pltpu.make_async_copy(partners, chosen, csem.at[1])
    for stage in stages[:AHEAD]:
        issue(stage)
    choose.start()
    load.start()
    for number, stage in enumerate(stages):
        arrive(stage)
        if number + AHEAD < len(stages):
            issue(stages[number + AHEAD])
        if ready[number] is not None:
            compute(ready[number])
    for stage in stages:
        for batch in stage:
            for to, _ in peers:
                outgoing(batch, to).wait_send()
            if batch[0] < 4:
                forward(batch).wait_send()
    reduce_terms(heads - 1)
    for head in range(max(heads - 2, 0), heads):
        for to, _ in groups:
            give_term(head, to, group).wait_send()
    for lot in lots:
        if lot is not None:
            for which in range(2):
                keep(lot, which).wait()
                for to, maker in peers:
                    give(lot, which, to).wait_send()
                    take(lot, which, maker).wait_recv()


def store_kernel(*refs):
    moves = [pltpu.make_async_copy(refs[i], refs[3 + i], refs[6].at[i]) for i in range(3)]
    for move in moves:
        move.start()
    for move in moves:
        move.wait()


def on_device(
    queries, key_rows, value_rows, query_tangent, key_tangent, value_tangent, partners, cotangent
):
    n, clips = lax.axis_size("head"), lax.axis_size("clip")
    rows, cols = queries.shape[0] * n, queries.shape[1] // n
    heads = cols // HDIM
    width = cotangent.shape[1]
    args = (key_rows, key_tangent, value_rows, value_tangent, query_tangent, queries)
    low, f32 = jnp.bfloat16, jnp.float32
    shapes = [(queries.shape, low), (queries.shape, low), ((width // clips, cols), f32)]
    dma = pltpu.SemaphoreType.DMA
    hbm, vmem = pl.BlockSpec(memory_space=pltpu.HBM), pl.BlockSpec(memory_space=pltpu.VMEM)
    results = pl.pallas_call(
        functools.partial(exchange_kernel, n, clips, heads),
        out_shape=tuple(pltpu.VMEM(*s) for s in shapes),
        in_specs=[hbm] * 8,
        out_specs=[vmem] * 3,
        scratch_shapes=[pltpu.VMEM((2 * rows, 2 * cols), low)] * 2
        + [pltpu.VMEM((rows, 2 * cols), low)] * 2
        + [pltpu.VMEM((3 * CLIP, 2 * HDIM), low)] * 2
        + [
            pltpu.VMEM((rows, width), low),
            pltpu.VMEM((HDIM, rows), low),
            pltpu.VMEM((2, HDIM, width), f32),
            pltpu.VMEM((heads, clips, HDIM, width // clips), f32),
            pltpu.SMEM(partners.shape[::-1], partners.dtype),
        ]
        + [dma((heads, 6, n)), dma((heads, 6, n)), dma((heads, 6)), dma((heads, 4)), dma((heads, 4))]
        + [dma((heads, 2, n)), dma((heads, 2, n)), dma((heads, 2))]
        + [dma((heads, clips)), dma((heads, clips)), dma((2,))],
        compiler_params=pltpu.CompilerParams(
            collective_id=0, has_side_effects=True, vmem_limit_bytes=58 * 1024 * 1024
        ),
        cost_estimate=pl.CostEstimate(
            flops=12 * rows * cols * 3 * CLIP + 2 * rows * cols * width,
            bytes_accessed=16 * rows * cols * 2 + rows * width * 2,
            transcendentals=rows * heads * 3 * CLIP,
        ),
    )(partners.T, *args, cotangent)
    return pl.pallas_call(
        store_kernel,
        out_shape=tuple(jax.ShapeDtypeStruct(*s) for s in shapes),
        in_specs=[vmem] * 3,
        out_specs=[hbm] * 3,
        scratch_shapes=[dma((3,))],
        compiler_params=pltpu.CompilerParams(vmem_limit_bytes=1024 * 1024),
    )(*(pltpu.with_memory_space_constraint(r, pltpu.VMEM) for r in results))


def solution(mesh):
    tokens = P(("clip", "head"), None)
    return jax.shard_map(
        on_device,
        mesh=mesh,
        in_specs=(tokens,) * 6 + (P(), P("clip", None)),
        out_specs=(tokens, tokens, P("clip", "head")),
        check_vma=False,
    )
```

```python
import functools
import math

import jax
import jax.numpy as jnp
from jax import lax
from jax.experimental import pallas as pl
from jax.experimental.pallas import tpu as pltpu
from jax.sharding import PartitionSpec as P

HDIM = 128
CLIP = 1024
AHEAD = 4
NT = (((1,), (1,)), ((), ()))
MESH = pl.DeviceIdType.MESH


def attend_rows(both, wk, wv, scale):
    f32 = jnp.float32
    scores = lax.dot_general(both[:, HDIM:], wk[:, :HDIM], NT, preferred_element_type=f32)
    score_tan = lax.dot_general(both, wk[...], NT, preferred_element_type=f32)
    row_max = jnp.max(scores, axis=1, keepdims=True)
    weights = jnp.exp2((scores - row_max) * (scale * math.log2(math.e)))
    inverse = 1.0 / jnp.sum(weights, axis=1, keepdims=True)
    mean = jnp.sum(weights * score_tan, axis=1, keepdims=True) * inverse
    low = weights.astype(jnp.bfloat16)
    tan_low = (weights * (score_tan - mean)).astype(jnp.bfloat16)
    first = jnp.dot(low, wv[...], preferred_element_type=f32)
    second = jnp.dot(tan_low, wv[:, :HDIM], preferred_element_type=f32)
    out = first[:, :HDIM] * inverse
    tan = (first[:, HDIM:] + second * scale) * inverse
    return out.astype(jnp.bfloat16), tan.astype(jnp.bfloat16)


def exchange_kernel(n, clips, heads, partners, *refs):
    args, cotangent, (out, tan, grad) = refs[:6], refs[6], refs[7:10]
    kk, vv, qq, oo, wk, wv, cot, flipped, terms, others, chosen = refs[10:21]
    send, recv, local, fsend, frecv, osend, orecv, olocal, gsend, grecv, csem = refs[21:]
    piece = args[0].shape[0]
    rows = n * piece
    wide = cot.shape[1] // clips
    me, group = lax.axis_index("head"), lax.axis_index("clip")
    after = lax.rem(group + 1, clips)
    if n & (n - 1) == 0:
        steps = [d for bit in range(n.bit_length() - 2, -1, -1) for d in range(1 << bit, 2 << bit)]
        peers = [(me ^ d, me ^ d) for d in steps]
    else:
        peers = [(lax.rem(me + d, n), lax.rem(me + n - d, n)) for d in range(1, n)]
    groups = [(lax.rem(group + d, clips), lax.rem(group + clips - d, clips)) for d in range(1, clips)]

    barrier = pltpu.get_barrier_semaphore()
    for to, _ in peers:
        pl.semaphore_signal(barrier, inc=1, device_id={"head": to}, device_id_type=MESH)
    for to, _ in groups:
        pl.semaphore_signal(barrier, inc=1, device_id={"clip": to}, device_id_type=MESH)
    pl.semaphore_wait(barrier, n - 1 + clips - 1)

    def whole(owner, head, count):
        return pl.ds(pl.multiple_of((owner * heads + head) * HDIM, HDIM), count * HDIM)

    def held(part, head, count):
        return pl.ds((heads * part + head) * HDIM, count * HDIM)

    def piece_of(base, source):
        return pl.ds(pl.multiple_of(base + source * piece, piece), piece)

    def landing(batch, source):
        t, head, count = batch
        buffer, base = ((kk, rows), (vv, rows), (qq, 0))[t // 2]
        return buffer.at[piece_of(base, source), held(t % 2, head, count)]

    def column(batch, owner):
        t, head, count = batch
        return args[t].at[:, whole(owner, head, count)]

    def outgoing(batch, to):
        t, head, count = batch
        return pltpu.make_async_remote_copy(
            src_ref=column(batch, to),
            dst_ref=landing(batch, me),
            send_sem=send.at[head, t, to],
            recv_sem=recv.at[head, t, me],
            device_id={"head": to},
            device_id_type=MESH,
        )

    def incoming(batch, source):
        t, head, count = batch
        return pltpu.make_async_remote_copy(
            src_ref=column(batch, source),
            dst_ref=landing(batch, source),
            send_sem=send.at[head, t, source],
            recv_sem=recv.at[head, t, source],
            device_id={"head": source},
            device_id_type=MESH,
        )

    def stay(batch):
        t, head, count = batch
        return pltpu.make_async_copy(column(batch, me), landing(batch, me), local.at[head, t])

    def forward(batch):
        t, head, count = batch
        buffer, cols = (kk, vv)[t // 2], held(t % 2, head, count)
        return pltpu.make_async_remote_copy(
            src_ref=buffer.at[pl.ds(rows, rows), cols],
            dst_ref=buffer.at[pl.ds(0, rows), cols],
            send_sem=fsend.at[head, t],
            recv_sem=frecv.at[head, t],
            device_id={"clip": after},
            device_id_type=MESH,
        )

    def issue(stage):
        for batch in stage:
            for to, _ in peers:
                outgoing(batch, to).start()
            stay(batch).start()

    def arrive(stage):
        for batch in stage:
            stay(batch).wait()
            for _, source in peers:
                incoming(batch, source).wait_recv()
            if batch[0] < 4:
                forward(batch).start()

    def result_rows(lot, which, owner):
        head, count = lot
        at = pl.ds(pl.multiple_of(owner * piece, piece), piece)
        return oo.at[at, held(which, head, count)]

    def result_home(lot, which, maker):
        return (out, tan)[which].at[:, whole(maker, *lot)]

    def give(lot, which, to):
        return pltpu.make_async_remote_copy(
            src_ref=result_rows(lot, which, to),
            dst_ref=result_home(lot, which, me),
            send_sem=osend.at[lot[0], which, to],
            recv_sem=orecv.at[lot[0], which, me],
            device_id={"head": to},
            device_id_type=MESH,
        )

    def take(lot, which, maker):
        return pltpu.make_async_remote_copy(
            src_ref=result_rows(lot, which, maker),
            dst_ref=result_home(lot, which, maker),
            send_sem=osend.at[lot[0], which, maker],
            recv_sem=orecv.at[lot[0], which, maker],
            device_id={"head": maker},
            device_id_type=MESH,
        )

    def keep(lot, which):
        return pltpu.make_async_copy(
            result_rows(lot, which, me), result_home(lot, which, me), olocal.at[lot[0], which]
        )

    def hand_out(lot, owner):
        @pl.when(owner == me)
        def _():
            for which in range(2):
                keep(lot, which).start()

        @pl.when(owner != me)
        def _():
            for which in range(2):
                give(lot, which, owner).start()

    clip_count = rows // CLIP
    block_rows = min(256, piece)
    per_clip, per_piece = CLIP // block_rows, piece // block_rows
    total_clips = clip_count * clips
    home = me * piece // CLIP

    def block_of(step):
        within = lax.rem(home + 1 + step // per_clip, clip_count)
        return within * per_clip + lax.rem(step, per_clip)

    def is_one(value):
        return jnp.full((16, HDIM), jnp.where(value, 1.0, 0.0), jnp.float32).astype(jnp.bfloat16)

    def attend(head, lot):
        def one_clip(turn, _):
            within = lax.rem(home + 1 + turn, clip_count)
            own = clip_count + within
            clip_id = group * clip_count + within
            gaps = [lax.rem(clip_id - chosen[i, clip_id] + total_clips, total_clips) for i in range(2)]
            near, far = jnp.minimum(*gaps) == 1, jnp.maximum(*gaps) == 2
            flags = [is_one(near), is_one(jnp.logical_not(near)), is_one(far), is_one(jnp.logical_not(far))]
            for place in range(3):
                at = pl.ds(place * CLIP, CLIP)
                for window, rows_held in ((wk, kk), (wv, vv)):
                    for part in range(2):

                        def clip_back(gap):
                            row = pl.multiple_of(lax.max(own - gap, 0) * CLIP, CLIP)
                            return rows_held[pl.ds(row, CLIP), held(part, head, 1)]

                        if place == 0:
                            mixed = clip_back(0)
                        else:
                            first, second = (
                                clip_back(place + i).reshape(CLIP // 16, 16, HDIM) * flags[place * 2 - 2 + i]
                                for i in range(2)
                            )
                            mixed = (first + second).reshape(CLIP, HDIM)
                        window[at, part * HDIM : (part + 1) * HDIM] = mixed

            def one_block(block, _):
                row = within * CLIP + block * block_rows
                at = pl.ds(pl.multiple_of(row, block_rows), block_rows)
                step = turn * per_clip + block
                both = jnp.concatenate([qq[at, held(part, head, 1)] for part in range(2)], axis=1)
                result = attend_rows(both, wk, wv, HDIM**-0.5)
                oo[at, held(0, head, 1)], oo[at, held(1, head, 1)] = result

                if lot is not None:

                    @pl.when(jnp.logical_and(step > 0, lax.rem(step, per_piece) == 0))
                    def _():
                        hand_out(lot, block_of(step - 1) // per_piece)

                return 0

            return lax.fori_loop(0, per_clip, one_block, 0)

        lax.fori_loop(0, clip_count, one_clip, 0)

    tile = 256 if cot.shape[1] % 256 == 0 else HDIM

    def multiply(head):
        flipped[...] = oo[:, held(0, head, 1)].T

        def one_tile(j, _):
            at = pl.ds(pl.multiple_of(j * tile, tile), tile)
            terms[head % 2, :, at] = jnp.dot(
                flipped[...], cot[:, at], preferred_element_type=jnp.float32
            )
            return 0

        lax.fori_loop(0, cot.shape[1] // tile, one_tile, 0)

    def share(owner):
        return pl.ds(pl.multiple_of(owner * wide, HDIM), wide)

    def give_term(head, to, source):
        return pltpu.make_async_remote_copy(
            src_ref=terms.at[head % 2, :, share(to)],
            dst_ref=others.at[head, source],
            send_sem=gsend.at[head, to],
            recv_sem=grecv.at[head, source],
            device_id={"clip": to},
            device_id_type=MESH,
        )

    def reduce_terms(head):
        total = terms[head % 2, :, share(group)]
        for _, source in groups:
            give_term(head, source, source).wait_recv()
            total = total + others[head, source]
        grad[:, head * HDIM : (head + 1) * HDIM] = total.T

    stages, ready = [], []
    for head in range(heads + 1):
        if head < heads:
            stages += [[(t, head, 1), (t + 1, head, 1)] for t in (0, 2)]
            ready += [None, None]
        if head:
            stages.append([(4, head - 1, 1), (5, head - 1, 1)])
            ready.append(head - 1)

    lots = [(i, 1) for i in range(heads)]
    if heads % 2 == 0:
        for i in range(0, heads - 2, 2):
            lots[i], lots[i + 1] = None, (i, 2)

    def compute(head):
        if head == 0:
            choose.wait()
            load.wait()
        for t in range(4):
            forward((t, head, 1)).wait_recv()
        attend(head, lots[head])
        if head >= 2:
            for to, _ in groups:
                give_term(head - 2, to, group).wait_send()
        multiply(head)
        if lots[head] is not None:
            hand_out(lots[head], block_of(rows // block_rows - 1) // per_piece)
        for to, _ in groups:
            give_term(head, to, group).start()
        if head:
            reduce_terms(head - 1)

    load = pltpu.make_async_copy(cotangent, cot, csem.at[0])
    choose = pltpu.make_async_copy(partners, chosen, csem.at[1])
    place = me // 2
    inner = jnp.logical_and(place > 0, place < n // 2 - 1)
    for stage in stages[:AHEAD]:
        issue(stage)

    @pl.when(inner)
    def _():
        for stage in stages[AHEAD:]:
            issue(stage)

    choose.start()
    load.start()
    for number, stage in enumerate(stages):
        arrive(stage)
        if number + AHEAD < len(stages):
            pl.when(jnp.logical_not(inner))(functools.partial(issue, stages[number + AHEAD]))
        if ready[number] is not None:
            compute(ready[number])
    for stage in stages:
        for batch in stage:
            for to, _ in peers:
                outgoing(batch, to).wait_send()
            if batch[0] < 4:
                forward(batch).wait_send()
    reduce_terms(heads - 1)
    for head in range(max(heads - 2, 0), heads):
        for to, _ in groups:
            give_term(head, to, group).wait_send()
    for lot in lots:
        if lot is not None:
            for which in range(2):
                keep(lot, which).wait()
                for to, maker in peers:
                    give(lot, which, to).wait_send()
                    take(lot, which, maker).wait_recv()


def store_kernel(*refs):
    moves = [pltpu.make_async_copy(refs[i], refs[3 + i], refs[6].at[i]) for i in range(3)]
    for move in moves:
        move.start()
    for move in moves:
        move.wait()


def on_device(
    queries, key_rows, value_rows, query_tangent, key_tangent, value_tangent, partners, cotangent
):
    n, clips = lax.axis_size("head"), lax.axis_size("clip")
    rows, cols = queries.shape[0] * n, queries.shape[1] // n
    heads = cols // HDIM
    width = cotangent.shape[1]
    args = (key_rows, key_tangent, value_rows, value_tangent, query_tangent, queries)
    low, f32 = jnp.bfloat16, jnp.float32
    shapes = [(queries.shape, low), (queries.shape, low), ((width // clips, cols), f32)]
    dma = pltpu.SemaphoreType.DMA
    hbm, vmem = pl.BlockSpec(memory_space=pltpu.HBM), pl.BlockSpec(memory_space=pltpu.VMEM)
    results = pl.pallas_call(
        functools.partial(exchange_kernel, n, clips, heads),
        out_shape=tuple(pltpu.VMEM(*s) for s in shapes),
        in_specs=[hbm] * 8,
        out_specs=[vmem] * 3,
        scratch_shapes=[pltpu.VMEM((2 * rows, 2 * cols), low)] * 2
        + [pltpu.VMEM((rows, 2 * cols), low)] * 2
        + [pltpu.VMEM((3 * CLIP, 2 * HDIM), low)] * 2
        + [
            pltpu.VMEM((rows, width), low),
            pltpu.VMEM((HDIM, rows), low),
            pltpu.VMEM((2, HDIM, width), f32),
            pltpu.VMEM((heads, clips, HDIM, width // clips), f32),
            pltpu.SMEM(partners.shape[::-1], partners.dtype),
        ]
        + [dma((heads, 6, n)), dma((heads, 6, n)), dma((heads, 6)), dma((heads, 4)), dma((heads, 4))]
        + [dma((heads, 2, n)), dma((heads, 2, n)), dma((heads, 2))]
        + [dma((heads, clips)), dma((heads, clips)), dma((2,))],
        compiler_params=pltpu.CompilerParams(
            collective_id=0, has_side_effects=True, vmem_limit_bytes=58 * 1024 * 1024
        ),
        cost_estimate=pl.CostEstimate(
            flops=12 * rows * cols * 3 * CLIP + 2 * rows * cols * width,
            bytes_accessed=16 * rows * cols * 2 + rows * width * 2,
            transcendentals=rows * heads * 3 * CLIP,
        ),
    )(partners.T, *args, cotangent)
    return pl.pallas_call(
        store_kernel,
        out_shape=tuple(jax.ShapeDtypeStruct(*s) for s in shapes),
        in_specs=[vmem] * 3,
        out_specs=[hbm] * 3,
        scratch_shapes=[dma((3,))],
        compiler_params=pltpu.CompilerParams(vmem_limit_bytes=1024 * 1024),
    )(*(pltpu.with_memory_space_constraint(r, pltpu.VMEM) for r in results))


def solution(mesh):
    tokens = P(("clip", "head"), None)
    return jax.shard_map(
        on_device,
        mesh=mesh,
        in_specs=(tokens,) * 6 + (P(), P("clip", None)),
        out_specs=(tokens, tokens, P("clip", "head")),
        check_vma=False,
    )
```

```python
import functools
import math

import jax
import jax.numpy as jnp
from jax import lax
from jax.experimental import pallas as pl
from jax.experimental.pallas import tpu as pltpu
from jax.sharding import PartitionSpec as P

HDIM = 128
CLIP = 1024
AHEAD = 4
NT = (((1,), (1,)), ((), ()))
MESH = pl.DeviceIdType.MESH


def attend_rows(both, wk, wv, scale):
    f32 = jnp.float32
    scores = lax.dot_general(both[:, HDIM:], wk[:, :HDIM], NT, preferred_element_type=f32)
    score_tan = lax.dot_general(both, wk[...], NT, preferred_element_type=f32)
    row_max = jnp.max(scores, axis=1, keepdims=True)
    weights = jnp.exp2((scores - row_max) * (scale * math.log2(math.e)))
    inverse = 1.0 / jnp.sum(weights, axis=1, keepdims=True)
    mean = jnp.sum(weights * score_tan, axis=1, keepdims=True) * inverse
    low = weights.astype(jnp.bfloat16)
    tan_low = (weights * (score_tan - mean)).astype(jnp.bfloat16)
    first = jnp.dot(low, wv[...], preferred_element_type=f32)
    second = jnp.dot(tan_low, wv[:, :HDIM], preferred_element_type=f32)
    out = first[:, :HDIM] * inverse
    tan = (first[:, HDIM:] + second * scale) * inverse
    return out.astype(jnp.bfloat16), tan.astype(jnp.bfloat16)


def exchange_kernel(n, clips, heads, partners, *refs):
    args, cotangent, (out, tan, grad) = refs[:6], refs[6], refs[7:10]
    kk, vv, qq, oo, wk, wv, cot, flipped, terms, others, chosen = refs[10:21]
    send, recv, local, fsend, frecv, osend, orecv, olocal, gsend, grecv, csem = refs[21:]
    piece = args[0].shape[0]
    rows = n * piece
    wide = cot.shape[1] // clips
    me, group = lax.axis_index("head"), lax.axis_index("clip")
    after = lax.rem(group + 1, clips)
    if n & (n - 1) == 0:
        steps = [d for bit in range(n.bit_length() - 2, -1, -1) for d in range(1 << bit, 2 << bit)]
        peers = [(me ^ d, me ^ d) for d in steps]
    else:
        peers = [(lax.rem(me + d, n), lax.rem(me + n - d, n)) for d in range(1, n)]
    groups = [(lax.rem(group + d, clips), lax.rem(group + clips - d, clips)) for d in range(1, clips)]

    barrier = pltpu.get_barrier_semaphore()
    for to, _ in peers:
        pl.semaphore_signal(barrier, inc=1, device_id={"head": to}, device_id_type=MESH)
    for to, _ in groups:
        pl.semaphore_signal(barrier, inc=1, device_id={"clip": to}, device_id_type=MESH)
    pl.semaphore_wait(barrier, n - 1 + clips - 1)

    def whole(owner, head, count):
        return pl.ds(pl.multiple_of((owner * heads + head) * HDIM, HDIM), count * HDIM)

    def held(part, head, count):
        return pl.ds((heads * part + head) * HDIM, count * HDIM)

    def piece_of(base, source):
        return pl.ds(pl.multiple_of(base + source * piece, piece), piece)

    def landing(batch, source):
        t, head, count = batch
        buffer, base = ((kk, rows), (vv, rows), (qq, 0))[t // 2]
        return buffer.at[piece_of(base, source), held(t % 2, head, count)]

    def column(batch, owner):
        t, head, count = batch
        return args[t].at[:, whole(owner, head, count)]

    def outgoing(batch, to):
        t, head, count = batch
        return pltpu.make_async_remote_copy(
            src_ref=column(batch, to),
            dst_ref=landing(batch, me),
            send_sem=send.at[head, t, to],
            recv_sem=recv.at[head, t, me],
            device_id={"head": to},
            device_id_type=MESH,
        )

    def incoming(batch, source):
        t, head, count = batch
        return pltpu.make_async_remote_copy(
            src_ref=column(batch, source),
            dst_ref=landing(batch, source),
            send_sem=send.at[head, t, source],
            recv_sem=recv.at[head, t, source],
            device_id={"head": source},
            device_id_type=MESH,
        )

    def stay(batch):
        t, head, count = batch
        return pltpu.make_async_copy(column(batch, me), landing(batch, me), local.at[head, t])

    def forward(batch):
        t, head, count = batch
        buffer, cols = (kk, vv)[t // 2], held(t % 2, head, count)
        return pltpu.make_async_remote_copy(
            src_ref=buffer.at[pl.ds(rows, rows), cols],
            dst_ref=buffer.at[pl.ds(0, rows), cols],
            send_sem=fsend.at[head, t],
            recv_sem=frecv.at[head, t],
            device_id={"clip": after},
            device_id_type=MESH,
        )

    def issue(stage):
        for batch in stage:
            for to, _ in peers:
                outgoing(batch, to).start()
            stay(batch).start()

    def arrive(stage):
        for batch in stage:
            stay(batch).wait()
            for _, source in peers:
                incoming(batch, source).wait_recv()
            if batch[0] < 4:
                forward(batch).start()

    def result_rows(lot, which, owner):
        head, count = lot
        at = pl.ds(pl.multiple_of(owner * piece, piece), piece)
        return oo.at[at, held(which, head, count)]

    def result_home(lot, which, maker):
        return (out, tan)[which].at[:, whole(maker, *lot)]

    def give(lot, which, to):
        return pltpu.make_async_remote_copy(
            src_ref=result_rows(lot, which, to),
            dst_ref=result_home(lot, which, me),
            send_sem=osend.at[lot[0], which, to],
            recv_sem=orecv.at[lot[0], which, me],
            device_id={"head": to},
            device_id_type=MESH,
        )

    def take(lot, which, maker):
        return pltpu.make_async_remote_copy(
            src_ref=result_rows(lot, which, maker),
            dst_ref=result_home(lot, which, maker),
            send_sem=osend.at[lot[0], which, maker],
            recv_sem=orecv.at[lot[0], which, maker],
            device_id={"head": maker},
            device_id_type=MESH,
        )

    def keep(lot, which):
        return pltpu.make_async_copy(
            result_rows(lot, which, me), result_home(lot, which, me), olocal.at[lot[0], which]
        )

    def hand_out(lot, owner):
        @pl.when(owner == me)
        def _():
            for which in range(2):
                keep(lot, which).start()

        @pl.when(owner != me)
        def _():
            for which in range(2):
                give(lot, which, owner).start()

    clip_count = rows // CLIP
    block_rows = min(256, piece)
    per_clip, per_piece = CLIP // block_rows, piece // block_rows
    total_clips = clip_count * clips
    home = me * piece // CLIP

    def block_of(step):
        within = lax.rem(home + 1 + step // per_clip, clip_count)
        return within * per_clip + lax.rem(step, per_clip)

    def is_one(value):
        return jnp.full((16, HDIM), jnp.where(value, 1.0, 0.0), jnp.float32).astype(jnp.bfloat16)

    def attend(head, lot):
        def one_clip(turn, _):
            within = lax.rem(home + 1 + turn, clip_count)
            own = clip_count + within
            clip_id = group * clip_count + within
            gaps = [lax.rem(clip_id - chosen[i, clip_id] + total_clips, total_clips) for i in range(2)]
            near, far = jnp.minimum(*gaps) == 1, jnp.maximum(*gaps) == 2
            flags = [is_one(near), is_one(jnp.logical_not(near)), is_one(far), is_one(jnp.logical_not(far))]
            for place in range(3):
                at = pl.ds(place * CLIP, CLIP)
                for window, rows_held in ((wk, kk), (wv, vv)):
                    for part in range(2):

                        def clip_back(gap):
                            row = pl.multiple_of(lax.max(own - gap, 0) * CLIP, CLIP)
                            return rows_held[pl.ds(row, CLIP), held(part, head, 1)]

                        if place == 0:
                            mixed = clip_back(0)
                        else:
                            first, second = (
                                clip_back(place + i).reshape(CLIP // 16, 16, HDIM) * flags[place * 2 - 2 + i]
                                for i in range(2)
                            )
                            mixed = (first + second).reshape(CLIP, HDIM)
                        window[at, part * HDIM : (part + 1) * HDIM] = mixed

            def one_block(block, _):
                row = within * CLIP + block * block_rows
                at = pl.ds(pl.multiple_of(row, block_rows), block_rows)
                step = turn * per_clip + block
                both = jnp.concatenate([qq[at, held(part, head, 1)] for part in range(2)], axis=1)
                result = attend_rows(both, wk, wv, HDIM**-0.5)
                oo[at, held(0, head, 1)], oo[at, held(1, head, 1)] = result

                if lot is not None:

                    @pl.when(jnp.logical_and(step > 0, lax.rem(step, per_piece) == 0))
                    def _():
                        hand_out(lot, block_of(step - 1) // per_piece)

                return 0

            return lax.fori_loop(0, per_clip, one_block, 0)

        lax.fori_loop(0, clip_count, one_clip, 0)

    tile = 256 if cot.shape[1] % 256 == 0 else HDIM

    def multiply(head):
        flipped[...] = oo[:, held(0, head, 1)].T

        def one_tile(j, _):
            at = pl.ds(pl.multiple_of(j * tile, tile), tile)
            terms[head % 2, :, at] = jnp.dot(
                flipped[...], cot[:, at], preferred_element_type=jnp.float32
            )
            return 0

        lax.fori_loop(0, cot.shape[1] // tile, one_tile, 0)

    def share(owner):
        return pl.ds(pl.multiple_of(owner * wide, HDIM), wide)

    def give_term(head, to, source):
        return pltpu.make_async_remote_copy(
            src_ref=terms.at[head % 2, :, share(to)],
            dst_ref=others.at[head, source],
            send_sem=gsend.at[head, to],
            recv_sem=grecv.at[head, source],
            device_id={"clip": to},
            device_id_type=MESH,
        )

    def reduce_terms(head):
        total = terms[head % 2, :, share(group)]
        for _, source in groups:
            give_term(head, source, source).wait_recv()
            total = total + others[head, source]
        grad[:, head * HDIM : (head + 1) * HDIM] = total.T

    stages, ready = [], []
    for head in range(heads + 1):
        if head < heads:
            stages += [[(t, head, 1), (t + 1, head, 1)] for t in (0, 2)]
            ready += [None, None]
        if heads >= 4 and head == 1:
            stages.append([(4, 0, 2), (5, 0, 2)])
            ready.append(0)
        elif heads >= 4 and head == 2:
            ready[-1] = 1
        elif head:
            stages.append([(4, head - 1, 1), (5, head - 1, 1)])
            ready.append(head - 1)

    lots = [(i, 1) for i in range(heads)]
    if heads % 2 == 0:
        for i in range(0, heads - 2, 2):
            lots[i], lots[i + 1] = None, (i, 2)

    def compute(head):
        if head == 0:
            choose.wait()
            load.wait()
        for t in range(4):
            forward((t, head, 1)).wait_recv()
        attend(head, lots[head])
        if head >= 2:
            for to, _ in groups:
                give_term(head - 2, to, group).wait_send()
        multiply(head)
        if lots[head] is not None:
            hand_out(lots[head], block_of(rows // block_rows - 1) // per_piece)
        for to, _ in groups:
            give_term(head, to, group).start()
        if head:
            reduce_terms(head - 1)

    load = pltpu.make_async_copy(cotangent, cot, csem.at[0])
    choose = pltpu.make_async_copy(partners, chosen, csem.at[1])
    for stage in stages[:AHEAD]:
        issue(stage)
    choose.start()
    load.start()
    for number, stage in enumerate(stages):
        arrive(stage)
        if number + AHEAD < len(stages):
            issue(stages[number + AHEAD])
        if ready[number] is not None:
            compute(ready[number])
    for stage in stages:
        for batch in stage:
            for to, _ in peers:
                outgoing(batch, to).wait_send()
            if batch[0] < 4:
                forward(batch).wait_send()
    reduce_terms(heads - 1)
    for head in range(max(heads - 2, 0), heads):
        for to, _ in groups:
            give_term(head, to, group).wait_send()
    for lot in lots:
        if lot is not None:
            for which in range(2):
                keep(lot, which).wait()
                for to, maker in peers:
                    give(lot, which, to).wait_send()
                    take(lot, which, maker).wait_recv()


def store_kernel(*refs):
    moves = [pltpu.make_async_copy(refs[i], refs[3 + i], refs[6].at[i]) for i in range(3)]
    for move in moves:
        move.start()
    for move in moves:
        move.wait()


def on_device(
    queries, key_rows, value_rows, query_tangent, key_tangent, value_tangent, partners, cotangent
):
    n, clips = lax.axis_size("head"), lax.axis_size("clip")
    rows, cols = queries.shape[0] * n, queries.shape[1] // n
    heads = cols // HDIM
    width = cotangent.shape[1]
    args = (key_rows, key_tangent, value_rows, value_tangent, query_tangent, queries)
    low, f32 = jnp.bfloat16, jnp.float32
    shapes = [(queries.shape, low), (queries.shape, low), ((width // clips, cols), f32)]
    dma = pltpu.SemaphoreType.DMA
    hbm, vmem = pl.BlockSpec(memory_space=pltpu.HBM), pl.BlockSpec(memory_space=pltpu.VMEM)
    results = pl.pallas_call(
        functools.partial(exchange_kernel, n, clips, heads),
        out_shape=tuple(pltpu.VMEM(*s) for s in shapes),
        in_specs=[hbm] * 8,
        out_specs=[vmem] * 3,
        scratch_shapes=[pltpu.VMEM((2 * rows, 2 * cols), low)] * 2
        + [pltpu.VMEM((rows, 2 * cols), low)] * 2
        + [pltpu.VMEM((3 * CLIP, 2 * HDIM), low)] * 2
        + [
            pltpu.VMEM((rows, width), low),
            pltpu.VMEM((HDIM, rows), low),
            pltpu.VMEM((2, HDIM, width), f32),
            pltpu.VMEM((heads, clips, HDIM, width // clips), f32),
            pltpu.SMEM(partners.shape[::-1], partners.dtype),
        ]
        + [dma((heads, 6, n)), dma((heads, 6, n)), dma((heads, 6)), dma((heads, 4)), dma((heads, 4))]
        + [dma((heads, 2, n)), dma((heads, 2, n)), dma((heads, 2))]
        + [dma((heads, clips)), dma((heads, clips)), dma((2,))],
        compiler_params=pltpu.CompilerParams(
            collective_id=0, has_side_effects=True, vmem_limit_bytes=58 * 1024 * 1024
        ),
        cost_estimate=pl.CostEstimate(
            flops=12 * rows * cols * 3 * CLIP + 2 * rows * cols * width,
            bytes_accessed=16 * rows * cols * 2 + rows * width * 2,
            transcendentals=rows * heads * 3 * CLIP,
        ),
    )(partners.T, *args, cotangent)
    return pl.pallas_call(
        store_kernel,
        out_shape=tuple(jax.ShapeDtypeStruct(*s) for s in shapes),
        in_specs=[vmem] * 3,
        out_specs=[hbm] * 3,
        scratch_shapes=[dma((3,))],
        compiler_params=pltpu.CompilerParams(vmem_limit_bytes=1024 * 1024),
    )(*(pltpu.with_memory_space_constraint(r, pltpu.VMEM) for r in results))


def solution(mesh):
    tokens = P(("clip", "head"), None)
    return jax.shard_map(
        on_device,
        mesh=mesh,
        in_specs=(tokens,) * 6 + (P(), P("clip", None)),
        out_specs=(tokens, tokens, P("clip", "head")),
        check_vma=False,
    )
```
